32 devices in a mesh: groups: 2 (over y), feat: 4 (over x, core), loop: 4 (over z).
Axes of the slice: x: 2, y: 2, z: 4, core: 2. Of those that a mesh axis runs over, the one named last changes fastest.
Arguments:
- train_grads: bfloat16 [512, 65536], P(('groups', 'loop'), 'feat'), parts along dimension 0, may hold values from -6 to 6
- query_grads: bfloat16 [64, 65536], P(('groups', 'loop'), 'feat'), parts along dimension 0, may hold values from -0.0234375 to 0.0234375
- curvature: float32 [65536], P('feat'), may hold values from 0.05 to 5
- row_counts: int32 [8], P(('groups', 'loop')), parts along dimension 0, may hold values from 1 to 64, 128 in all
Outputs:
- scores: float32 [512, 32], P(('groups', 'loop', 'feat')), parts along dimension 0
The draws below stay inside these ranges and needn't reach their ends.
There are 2 independent parts, one for each index of `groups`. The reference program is written for one: setup_inputs(seed, part) draws one part's arguments, and reference() takes and returns one part's arrays. A program takes and returns all parts, laid end to end along the dimension named above; an argument that names none is the same for every part. Nothing has to cross between parts.
Inputs may be any that keep to these rules, and one draw needn't show every extreme that they name: row_counts[s] is the number of live slots of loop shard s; slots 0 to row_counts[s] - 1 of that shard are live; some shard has exactly 64; the counts sum to 128.
All inputs are finite; a program needn't handle non-finite values.
Results may differ from the reference program's by a relative error of at most 0.0029.
Values may be sent and summed in bfloat16 or wider, within the bound.
A program may use at most 128 MiB of HBM per device.

```python
import math
import jax
import jax.numpy as jnp
import numpy as np

F = 65536
CAP = 64
TRAIN = 256
QUERIES = 32
N_LOOP = 4


def level_of(key, shape, split, low, top_value):
    loudness, own = 1.0, jax.random.fold_in(key, 6)
    for axis_at, parts in split:
        draws = jnp.exp(jax.random.uniform(jax.random.fold_in(own, axis_at), (parts,), jnp.float32, low / len(split), top_value / len(split)))
        loudness = loudness * jnp.repeat(draws, shape[axis_at] // parts).reshape([-1 if axis == axis_at else 1 for axis in range(len(shape))])
    return loudness


def profile(number_of, total, reach, lean):
    weights = [(1 << 20) // math.isqrt(grade ** lean) + 1 for grade in range(2, number_of + 1)]
    rest, counts = total - reach - (number_of - 1), [1] * (number_of - 1)
    while rest > 0:
        movable = [i for i in range(number_of - 1) if counts[i] < reach]
        mass, left = sum([weights[i] for i in movable]), rest
        for i in movable:
            addition = min(reach - counts[i], max(1, left * weights[i] // mass), rest)
            counts[i] = counts[i] + addition
            rest = rest - addition
    return np.array([reach] + counts)


def ragged_sizes(stream_key, count, total, reach, lean):
    if count == 2:
        one = jax.random.randint(stream_key, (), max(1, total - reach), min(reach, total - 1) + 1)
        return jnp.stack([one, total - one])
    tallies = jnp.asarray(profile(count, total, reach, lean), jnp.int32)
    pairs = (count - 1) // 2
    giver, receiver = tallies[1:1 + 2 * pairs:2], tallies[2:2 + 2 * pairs:2]
    room = jnp.minimum(giver - 1, reach - receiver)
    shifted = jax.random.randint(jax.random.fold_in(stream_key, 1), (pairs,), 0, 1 << 20) % (room + 1)
    tallies = tallies.at[1:1 + 2 * pairs:2].set(giver - shifted).at[2:2 + 2 * pairs:2].set(receiver + shifted)
    return tallies[jax.random.permutation(jax.random.fold_in(stream_key, 2), count)]


def bell_draw(own_key, dims, spread, bound, shards=(), kind=jnp.bfloat16):
    drawn = jax.random.normal(own_key, dims, jnp.float32) * spread
    if len(shards) > 0:
        drawn = level_of(own_key, dims, shards, -0.22, 0.18) * drawn
    return jnp.clip(drawn, min=-bound, max=bound).astype(kind)


def setup_inputs(seed: int = 0, part: int = 0) -> dict:
    key_of = jax.random.split(jax.random.key(seed), 5)
    part_keys = jax.random.split(jax.random.fold_in(key_of[4], part), 5)
    return {
        "train_grads": bell_draw(part_keys[0], (TRAIN, F), 1.0, 6.0, ((0, 4), (1, 4))),
        "query_grads": bell_draw(part_keys[1], (QUERIES, F), F ** -0.5, 0.0234375, ((0, 4), (1, 4))),
        "curvature": jnp.clip(jnp.exp(math.log(5.0) - 4.6051702 * jax.random.uniform(key_of[2], (F,), jnp.float32) ** level_of(key_of[2], (F,), ((0, 4),), -0.2, 0.2)), 0.05, 5.0),
        "row_counts": ragged_sizes(part_keys[3], N_LOOP, N_LOOP * CAP // 2, CAP, 2).astype(jnp.int32),
    }


damping_term = 0.1


def reference(train_grads, query_grads, curvature, row_counts):
    precond = (query_grads.astype(jnp.float32) / (damping_term + curvature[None, :])).astype(jnp.bfloat16)
    slots = jnp.arange(TRAIN, dtype=jnp.int32)
    shard_of = (slots // CAP).astype(jnp.int32)
    live = (slots % CAP) < row_counts[shard_of]
    raw = jnp.dot(train_grads, precond.T, preferred_element_type=jnp.float32)
    return jnp.where(live[:, None], raw, jnp.float32(0.0))
```

```python
import functools

import jax
import jax.numpy as jnp
from jax import lax
from jax.experimental import pallas as pl
from jax.experimental.pallas import tpu as pltpu
from jax.sharding import PartitionSpec as P

MESH = pl.DeviceIdType.MESH
damping_term = 0.1


def kernel(
    n, nf, cuts, split,
    t_hbm, q_hbm, c_hbm, count_ref, out_ref,
    gath, t_ref, c_ref, inv_ref, acc, part, red, t_tail, p_tail, tail_acc, tail_part,
    local_sem, recv_sem, share_sem, give_sem, ready_sem,
):
    me, f = lax.axis_index("loop"), lax.axis_index("feat")
    rows, width = t_ref.shape
    own_rows = rows // nf
    q_rows = gath.shape[1]
    pieces = len(cuts) - 1
    sizes = [cuts[p + 1] - cuts[p] for p in range(pieces)]
    mid, last = pieces - 2, pieces - 1
    has_left, has_right = me > 0, me < n - 1
    is_end = (me == 0) | (me == n - 1)
    is_helper = (me == 1) | (me == n - 2)
    even = lax.rem(f, 2) == 0

    def tail_here(piece):
        if not split or piece < mid:
            return False
        return True if piece == last else even

    load_q = [
        pltpu.make_async_copy(
            q_hbm.at[:, pl.ds(a, b - a)], gath.at[me, :, pl.ds(a, b - a)], local_sem.at[i]
        )
        for i, (a, b) in enumerate(((0, cuts[1]), (cuts[1], width)))
    ]
    load_c = pltpu.make_async_copy(c_hbm, c_ref, local_sem.at[3])
    load_t = pltpu.make_async_copy(t_hbm, t_ref, local_sem.at[2])
    for load in load_q:
        load.start()

    barrier = pltpu.get_barrier_semaphore()

    @pl.when(has_right)
    def _():
        pl.semaphore_signal(barrier, inc=1, device_id={"loop": me + 1}, device_id_type=MESH)

    for k in range(1, nf):
        pl.semaphore_signal(
            barrier, inc=1, device_id={"feat": lax.rem(f + k, nf)}, device_id_type=MESH
        )
    load_c.start()
    load_t.start()

    def columns(piece):
        return pl.ds(cuts[piece], sizes[piece])

    def hop(way, block, piece, taker):
        span = gath.at[block, :, columns(piece)]
        slot = block - (block > taker).astype(jnp.int32)
        return pltpu.make_async_remote_copy(
            src_ref=span,
            dst_ref=span,
            send_sem=local_sem.at[way],
            recv_sem=recv_sem.at[slot * pieces + piece],
            device_id={"loop": jnp.clip(me + (2 * way - 1), 0, n - 1)},
            device_id_type=MESH,
        )

    def goes(way, piece):
        there = has_right if way else has_left
        inner = me < n - 2 if way else me > 1
        tail = tail_here(piece)
        if tail is False:
            return there
        return inner if tail is True else there & (inner | jnp.logical_not(tail))

    def give(piece):
        at = pl.ds(cuts[piece] - cuts[mid], sizes[piece])
        return pltpu.make_async_remote_copy(
            src_ref=t_ref.at[:, columns(piece)],
            dst_ref=t_tail.at[:, at],
            send_sem=local_sem.at[3],
            recv_sem=give_sem.at[piece - mid],
            device_id={"loop": jnp.where(me == 0, 1, n - 2)},
            device_id_type=MESH,
        )

    def multiply(block, piece):
        here = pl.ds(pl.multiple_of(block * q_rows, q_rows), q_rows)
        exact = gath[block, :, columns(piece)].astype(jnp.float32) * inv_ref[:, columns(piece)]
        acc[here, 0:rows] += lax.dot_general(
            exact.astype(jnp.bfloat16), t_ref[:, columns(piece)], (((1,), (1,)), ((), ())),
            preferred_element_type=jnp.float32,
        )
        if split and piece >= mid:
            p_tail[here, pl.ds(cuts[piece] - cuts[mid], sizes[piece])] = exact

    mains = [(piece, True if tail_here(piece) is False else jnp.logical_not(even))
             for piece in range(pieces) if tail_here(piece) is not True]
    tails = [(piece, tail_here(piece)) for piece in range(pieces) if tail_here(piece) is not False]

    def take(way, block, piece):
        hop(way, block, piece, me).wait_recv()

        @pl.when(goes(way, piece))
        def _():
            hop(way, block, piece, me + 2 * way - 1).start()

    def arrive(back, piece, applies):
        from_left, from_right = me - back, me + back
        takes_left, takes_right = (from_left >= 0) & applies, (from_right < n) & applies
        moved = back > 0

        @pl.when(takes_right & moved)
        def _():
            take(0, from_right, piece)

        @pl.when(takes_left & moved)
        def _():
            take(1, from_left, piece)

        @pl.loop(0, 2)
        def _(side):
            @pl.when(((side == 0) & takes_left) | ((side == 1) & takes_right & moved))
            def _():
                multiply(me + (2 * side - 1) * back, piece)

    def own_mains(way):
        for piece, applies in mains:
            @pl.when(goes(way, piece) & applies)
            def _():
                hop(way, me, piece, me + 2 * way - 1).start()

    def own_tails(way):
        for piece, applies in tails:
            @pl.when(goes(way, piece) & applies)
            def _():
                hop(way, me, piece, me + 2 * way - 1).start()

    def arrive_tails(way, count):
        own_tails(way)

        @pl.loop(1, count + 1)
        def _(back):
            block = me + (1 - 2 * way) * back
            for piece, applies in tails:
                @pl.when(applies)
                def _():
                    take(way, block, piece)
                    multiply(block, piece)

    acc[...] = jnp.zeros_like(acc)
    pl.semaphore_wait(barrier, has_left.astype(jnp.int32) + nf - 1)

    @pl.when(has_left)
    def _():
        pl.semaphore_signal(ready_sem, inc=1, device_id={"loop": me - 1}, device_id_type=MESH)

    load_q[0].wait()

    @pl.when(has_left)
    def _():
        hop(0, me, 0, me - 1).start()

    load_q[1].wait()

    @pl.when(has_left)
    def _():
        for piece, applies in mains[1:]:
            @pl.when(goes(0, piece) & applies)
            def _():
                hop(0, me, piece, me - 1).start()

    if split:
        @pl.when(me == n - 1)
        def _():
            own_tails(0)

    @pl.when(has_right)
    def _():
        pl.semaphore_wait(ready_sem, 1)
        own_mains(1)

    if split:
        @pl.when(me == 0)
        def _():
            own_tails(1)

    load_c.wait()
    load_t.wait()
    if split:
        @pl.when(is_end & even)
        def _():
            give(mid).start()
            give(last).start()

    inv_ref[...] = 1.0 / (damping_term + c_ref[...])

    @pl.loop(0, n)
    def _(back):
        for piece, applies in mains:
            arrive(back, piece, applies)
            if split and piece == GIVE_PIECE:
                @pl.when(is_end & jnp.logical_not(even) & (back == n - GIVE_BACK))
                def _():
                    give(last).start()

        if split:
            @pl.when((back == 0) & jnp.logical_not(is_end))
            def _():
                for piece, applies in tails:
                    @pl.when(applies)
                    def _():
                        multiply(me, piece)

            for way in range(2):
                count = me if way else n - 1 - me

                @pl.when((back == count) & jnp.logical_not(is_end))
                def _():
                    arrive_tails(way, count)

    turned = acc[...].T
    for k in range(nf):
        part[k] = turned[k * own_rows:(k + 1) * own_rows, 0:part.shape[2]]

    def share(k):
        peer = lax.rem(f + k, nf)
        return pltpu.make_async_remote_copy(
            src_ref=part.at[peer],
            dst_ref=red.at[k - 1],
            send_sem=local_sem.at[2],
            recv_sem=share_sem.at[0],
            device_id={"feat": peer},
            device_id_type=MESH,
        )

    def tail_share(k):
        peer = lax.rem(f + k, nf)
        return pltpu.make_async_remote_copy(
            src_ref=tail_part.at[peer],
            dst_ref=red.at[nf - 1 + k],
            send_sem=local_sem.at[2],
            recv_sem=share_sem.at[0],
            device_id={"feat": peer, "loop": jnp.where(me == 1, 0, n - 1)},
            device_id_type=MESH,
        )

    for k in range(1, nf):
        share(k).start()

    def tail_dot(piece):
        at = pl.ds(cuts[piece] - cuts[mid], sizes[piece])
        return lax.dot_general(
            t_tail[:, at], p_tail[:, at].astype(jnp.bfloat16), (((1,), (1,)), ((), ())),
            preferred_element_type=jnp.float32,
        )

    def hand_over(total):
        for k in range(nf):
            tail_part[k] = total[k * own_rows:(k + 1) * own_rows, :]
        for k in range(nf):
            tail_share(k).start()

    if split:
        @pl.when(is_helper & even)
        def _():
            give(mid).wait_recv()
            tail_acc[...] = tail_dot(mid)
            give(last).wait_recv()
            hand_over(tail_acc[...] + tail_dot(last))

        @pl.when(is_helper & jnp.logical_not(even))
        def _():
            give(last).wait_recv()
            hand_over(tail_dot(last))

    def sent(way, blocks, wide):
        span = gath.at[pl.ds(0, blocks), :, pl.ds(0, wide)]
        pltpu.make_async_remote_copy(
            src_ref=span,
            dst_ref=span,
            send_sem=local_sem.at[way],
            recv_sem=recv_sem.at[0],
            device_id={"loop": jnp.clip(me + (2 * way - 1), 0, n - 1)},
            device_id_type=MESH,
        ).wait_send()

    for blocks in range(1, n):
        for way in range(2):
            at = me == (blocks - 1 if way else n - blocks)
            if not split or blocks < n - 1:
                @pl.when(at)
                def _():
                    sent(way, blocks, width)
            else:
                for wide, which in ((cuts[mid], even), (cuts[last], jnp.logical_not(even))):
                    @pl.when(at & which)
                    def _():
                        sent(way, blocks, wide)

    if split:
        for start, which in ((mid, even), (last, jnp.logical_not(even))):
            @pl.when(is_end & which)
            def _():
                span = pl.ds(cuts[start], width - cuts[start])
                pltpu.make_async_remote_copy(
                    src_ref=t_ref.at[:, span],
                    dst_ref=t_ref.at[:, span],
                    send_sem=local_sem.at[3],
                    recv_sem=give_sem.at[0],
                    device_id={"loop": jnp.where(me == 0, 1, n - 2)},
                    device_id_type=MESH,
                ).wait_send()

    def shares_in(count):
        pltpu.make_async_remote_copy(
            src_ref=red.at[pl.ds(0, count)],
            dst_ref=red.at[pl.ds(0, count)],
            send_sem=local_sem.at[2],
            recv_sem=share_sem.at[0],
            device_id={"feat": lax.rem(f + 1, nf)},
            device_id_type=MESH,
        ).wait_recv()

    def shares_out(count):
        pltpu.make_async_remote_copy(
            src_ref=red.at[pl.ds(0, count)],
            dst_ref=red.at[pl.ds(0, count)],
            send_sem=local_sem.at[2],
            recv_sem=share_sem.at[0],
            device_id={"feat": lax.rem(f + 1, nf)},
            device_id_type=MESH,
        ).wait_send()

    live = f * own_rows + lax.broadcasted_iota(jnp.int32, out_ref.shape, 0) < count_ref[0]

    def finish(count):
        shares_in(count)
        total = part[f]
        for k in range(count):
            total = total + red[k]
        out_ref[...] = jnp.where(live, total, 0.0)

    if split:
        @pl.when(is_end)
        def _():
            finish(2 * nf - 1)

        @pl.when(jnp.logical_not(is_end))
        def _():
            finish(nf - 1)

        @pl.when(is_helper)
        def _():
            shares_out(2 * nf - 1)

        @pl.when(jnp.logical_not(is_helper))
        def _():
            shares_out(nf - 1)
    else:
        finish(nf - 1)
        shares_out(nf - 1)


GIVE_PIECE = 2
GIVE_BACK = 2
EVEN_TAIL = 29
ODD_TAIL = 9


def on_device(n, nf, train_grads, query_grads, curvature, row_counts):
    rows, width = train_grads.shape
    q_rows = query_grads.shape[0]
    queries = n * q_rows
    split = n >= 4
    even_tail = width * EVEN_TAIL // 128 // 128 * 128
    odd_tail = width * ODD_TAIL // 128 // 128 * 128
    main = width - even_tail
    cuts = [main * i // 4 // 128 * 128 for i in range(4)] + [main, width - odd_tail, width]
    lanes = -(-rows // 128) * 128
    tail = width - main
    hbm = pl.BlockSpec(memory_space=pltpu.HBM)
    return pl.pallas_call(
        functools.partial(kernel, n, nf, cuts, split),
        out_shape=pltpu.VMEM((rows // nf, queries), jnp.float32),
        in_specs=[hbm] * 3 + [pl.BlockSpec(memory_space=pltpu.SMEM)],
        out_specs=pl.BlockSpec(memory_space=pltpu.VMEM),
        scratch_shapes=[
            pltpu.VMEM((n, q_rows, width), jnp.bfloat16),
            pltpu.VMEM((rows, width), jnp.bfloat16),
            pltpu.VMEM((1, width), jnp.float32),
            pltpu.VMEM((1, width), jnp.float32),
            pltpu.VMEM((queries, lanes), jnp.float32),
            pltpu.VMEM((nf, rows // nf, queries), jnp.float32),
            pltpu.VMEM((2 * nf - 1, rows // nf, queries), jnp.float32),
            pltpu.VMEM((rows, tail), jnp.bfloat16),
            pltpu.VMEM((queries, tail), jnp.float32),
            pltpu.VMEM((rows, queries), jnp.float32),
            pltpu.VMEM((nf, rows // nf, queries), jnp.float32),
            pltpu.SemaphoreType.DMA((4,)),
            pltpu.SemaphoreType.DMA(((n - 1) * (len(cuts) - 1),)),
            pltpu.SemaphoreType.DMA((1,)),
            pltpu.SemaphoreType.DMA((2,)),
            pltpu.SemaphoreType.REGULAR,
        ],
        compiler_params=pltpu.CompilerParams(collective_id=0, has_side_effects=True),
    )(train_grads, query_grads, curvature.reshape(1, width), row_counts)


def solution(mesh):
    placed = (
        P(("groups", "loop"), "feat"),
        P(("groups", "loop"), "feat"),
        P("feat"),
        P(("groups", "loop")),
    )
    return jax.shard_map(
        functools.partial(on_device, mesh.shape["loop"], mesh.shape["feat"]),
        mesh=mesh,
        in_specs=placed,
        out_specs=P(("groups", "loop", "feat"), None),
        check_vma=False,
    )
```

```python
import functools

import jax
import jax.numpy as jnp
from jax import lax
from jax.experimental import pallas as pl
from jax.experimental.pallas import tpu as pltpu
from jax.sharding import PartitionSpec as P

MESH = pl.DeviceIdType.MESH
damping_term = 0.1
MAINS = ((21, 42, 63, 84, 96), (24, 48, 72, 96, 116))
GIVES = ((116, 128), (128,))
GIVE_AT = (None, (2, 3))
UNITS = 128


def kernel(
    n, nf, mains, gives, give_at,
    t_hbm, q_hbm, c_hbm, count_ref, out_ref,
    q_ref, gath, t_ref, c_ref, inv_ref, acc, part, red, t_tail, p_tail, tail_acc, tail_part,
    local_sem, recv_sem, share_sem, give_sem, ready_sem,
):
    me, f = lax.axis_index("loop"), lax.axis_index("feat")
    rows, width = t_ref.shape
    own_rows = rows // nf
    q_rows = q_ref.shape[0]
    slots = max(len(cuts) for cuts in mains)
    has_left, has_right = me > 0, me < n - 1
    is_first = me == 0
    is_end = is_first | (me == n - 1)
    is_helper = (me == 1) | (me == n - 2)
    head = max(cuts[1] for cuts in mains)

    load_q = [
        pltpu.make_async_copy(
            q_hbm.at[:, pl.ds(a, b - a)], q_ref.at[:, pl.ds(a, b - a)], local_sem.at[i]
        )
        for i, (a, b) in enumerate(((0, head), (head, width)))
    ]
    load_c = pltpu.make_async_copy(c_hbm, c_ref, local_sem.at[3])
    load_t = pltpu.make_async_copy(t_hbm, t_ref, local_sem.at[2])
    for load in load_q:
        load.start()

    barrier = pltpu.get_barrier_semaphore()

    @pl.when(has_right)
    def _():
        pl.semaphore_signal(barrier, inc=1, device_id={"loop": me + 1}, device_id_type=MESH)

    @pl.when(me == 1)
    def _():
        pl.semaphore_signal(barrier, inc=1, device_id={"loop": me - 1}, device_id_type=MESH)

    for k in range(1, nf):
        pl.semaphore_signal(
            barrier, inc=1, device_id={"feat": lax.rem(f + k, nf)}, device_id_type=MESH
        )
    load_c.start()
    load_t.start()
    acc[...] = jnp.zeros_like(acc)
    pl.semaphore_wait(barrier, jnp.where(is_first, has_right, has_left).astype(jnp.int32) + nf - 1)

    @pl.when(me > 1)
    def _():
        pl.semaphore_signal(ready_sem, inc=1, device_id={"loop": me - 1}, device_id_type=MESH)

    load_q[0].wait()

    def share(k):
        peer = lax.rem(f + k, nf)
        return pltpu.make_async_remote_copy(
            src_ref=part.at[peer],
            dst_ref=red.at[k - 1],
            send_sem=local_sem.at[2],
            recv_sem=share_sem.at[0],
            device_id={"feat": peer},
            device_id_type=MESH,
        )

    def tail_share(k):
        peer = lax.rem(f + k, nf)
        return pltpu.make_async_remote_copy(
            src_ref=tail_part.at[peer],
            dst_ref=red.at[nf - 1 + k],
            send_sem=local_sem.at[2],
            recv_sem=share_sem.at[0],
            device_id={"feat": peer, "loop": jnp.where(me == 1, 0, n - 1)},
            device_id_type=MESH,
        )

    def all_shares(count):
        return pltpu.make_async_remote_copy(
            src_ref=red.at[pl.ds(0, count)],
            dst_ref=red.at[pl.ds(0, count)],
            send_sem=local_sem.at[2],
            recv_sem=share_sem.at[0],
            device_id={"feat": lax.rem(f + 1, nf)},
            device_id_type=MESH,
        )

    def run(cuts, gift, give_when):
        count = len(cuts) - 1
        main = cuts[-1]
        tail = main < width

        def columns(piece):
            a = cuts[piece]
            b = cuts[piece + 1] if piece < count else width
            return pl.ds(a, b - a)

        def hop(way, block, piece, taker, own=False):
            span = gath.at[block, :, columns(piece)]
            slot = block - (block > taker).astype(jnp.int32)
            return pltpu.make_async_remote_copy(
                src_ref=q_ref.at[:, columns(piece)] if own else span,
                dst_ref=span,
                send_sem=local_sem.at[way],
                recv_sem=recv_sem.at[slot * slots + piece],
                device_id={"loop": jnp.clip(me + (2 * way - 1), 0, n - 1)},
                device_id_type=MESH,
            )

        def goes(way, piece):
            if piece < count:
                return has_right if way else has_left
            return me < n - 2 if way else me > 1

        def send_own(way, pieces):
            @pl.when(goes(way, pieces[0]))
            def _():
                for piece in pieces:
                    hop(way, me, piece, me + 2 * way - 1, own=True).start()

        def give(i):
            a, b = gift[i], gift[i + 1]
            return pltpu.make_async_remote_copy(
                src_ref=t_ref.at[:, pl.ds(a, b - a)],
                dst_ref=t_tail.at[:, pl.ds(a - main, b - a)],
                send_sem=local_sem.at[3],
                recv_sem=give_sem.at[i],
                device_id={"loop": jnp.where(is_first, 1, n - 2)},
                device_id_type=MESH,
            )

        def start_give():
            for i in range(len(gift) - 1):
                give(i).start()

        def multiply(block, piece, own=False):
            here = pl.ds(pl.multiple_of(block * q_rows, q_rows), q_rows)
            held = q_ref[:, columns(piece)] if own else gath[block, :, columns(piece)]
            exact = held.astype(jnp.float32) * inv_ref[:, columns(piece)]
            acc[here, 0:rows] += lax.dot_general(
                exact.astype(jnp.bfloat16), t_ref[:, columns(piece)], (((1,), (1,)), ((), ())),
                preferred_element_type=jnp.float32,
            )
            if piece == count:
                p_tail[here, 0:width - main] = exact

        def take(way, block, piece):
            hop(way, block, piece, me).wait_recv()

            @pl.when(goes(way, piece))
            def _():
                hop(way, block, piece, me + 2 * way - 1).start()

        def arrive(back, piece):
            from_left, from_right = me - back, me + back
            takes_left, takes_right = from_left >= 0, from_right < n

            @pl.when(takes_right)
            def _():
                take(0, from_right, piece)

            @pl.when(takes_left)
            def _():
                take(1, from_left, piece)

            @pl.loop(0, 2)
            def _(side):
                @pl.when(((side == 0) & takes_left) | ((side == 1) & takes_right))
                def _():
                    multiply(me + (2 * side - 1) * back, piece)

        send_own(0, [0])
        load_q[1].wait()
        send_own(0, range(1, count))
        if tail:
            @pl.when(me == n - 1)
            def _():
                send_own(0, [count])

        @pl.when(has_right & jnp.logical_not(is_first))
        def _():
            pl.semaphore_wait(ready_sem, 1)

        send_own(1, range(count))
        if tail:
            @pl.when(is_first)
            def _():
                send_own(1, [count])

        load_c.wait()
        load_t.wait()
        if tail and give_when is None:
            @pl.when(is_end)
            def _():
                start_give()

        inv_ref[...] = 1.0 / (damping_term + c_ref[...])
        for piece in range(count):
            multiply(me, piece, own=True)
        if tail:
            @pl.when(jnp.logical_not(is_end))
            def _():
                multiply(me, count, own=True)

        @pl.loop(1, n)
        def _(back):
            for piece in range(count):
                arrive(back, piece)
                if tail and give_when is not None and piece == give_when[1]:
                    @pl.when(is_end & (back == n - give_when[0]))
                    def _():
                        start_give()

            if tail:
                for way in range(2):
                    deep = me if way else n - 1 - me

                    @pl.when((back == deep) & jnp.logical_not(is_end))
                    def _():
                        send_own(way, [count])

                        @pl.loop(1, deep + 1)
                        def _(far):
                            block = me + (1 - 2 * way) * far
                            take(way, block, count)
                            multiply(block, count)

        turned = acc[...].T
        for k in range(nf):
            part[k] = turned[k * own_rows:(k + 1) * own_rows, 0:part.shape[2]]
        for k in range(1, nf):
            share(k).start()

        def tail_dot(i):
            at = pl.ds(gift[i] - main, gift[i + 1] - gift[i])
            return lax.dot_general(
                t_tail[:, at], p_tail[:, at].astype(jnp.bfloat16), (((1,), (1,)), ((), ())),
                preferred_element_type=jnp.float32,
            )

        if tail:
            @pl.when(is_helper)
            def _():
                total = None
                for i in range(len(gift) - 1):
                    give(i).wait_recv()
                    total = tail_dot(i) if total is None else tail_acc[...] + tail_dot(i)
                    if i < len(gift) - 2:
                        tail_acc[...] = total
                for k in range(nf):
                    tail_part[k] = total[k * own_rows:(k + 1) * own_rows, :]
                for k in range(nf):
                    tail_share(k).start()

        def sent(way, blocks, wide):
            span = gath.at[pl.ds(0, blocks), :, pl.ds(0, wide)]
            pltpu.make_async_remote_copy(
                src_ref=span,
                dst_ref=span,
                send_sem=local_sem.at[way],
                recv_sem=recv_sem.at[0],
                device_id={"loop": jnp.clip(me + (2 * way - 1), 0, n - 1)},
                device_id_type=MESH,
            ).wait_send()

        for blocks in range(1, n):
            for way in range(2):
                @pl.when(me == (blocks - 1 if way else n - blocks))
                def _():
                    sent(way, blocks, width if blocks < n - 1 else main)

        if tail:
            @pl.when(is_end)
            def _():
                span = t_ref.at[:, pl.ds(main, width - main)]
                pltpu.make_async_remote_copy(
                    src_ref=span,
                    dst_ref=span,
                    send_sem=local_sem.at[3],
                    recv_sem=give_sem.at[0],
                    device_id={"loop": jnp.where(is_first, 1, n - 2)},
                    device_id_type=MESH,
                ).wait_send()

    if mains[0] == mains[1]:
        run(mains[0], gives[0], give_at[0])
    else:
        for parity in range(2):
            @pl.when(lax.rem(f, 2) == parity)
            def _():
                run(mains[parity], gives[parity], give_at[parity])

    live = f * own_rows + lax.broadcasted_iota(jnp.int32, out_ref.shape, 0) < count_ref[0]

    def finish(count):
        all_shares(count).wait_recv()
        total = part[f]
        for k in range(count):
            total = total + red[k]
        out_ref[...] = jnp.where(live, total, 0.0)

    if mains[0][-1] == width:
        finish(nf - 1)
        all_shares(nf - 1).wait_send()
    else:
        @pl.when(is_end)
        def _():
            finish(2 * nf - 1)

        @pl.when(jnp.logical_not(is_end))
        def _():
            finish(nf - 1)

        @pl.when(is_helper)
        def _():
            all_shares(2 * nf - 1).wait_send()

        @pl.when(jnp.logical_not(is_helper))
        def _():
            all_shares(nf - 1).wait_send()


def on_device(n, nf, train_grads, query_grads, curvature, row_counts):
    rows, width = train_grads.shape
    q_rows = query_grads.shape[0]
    queries = n * q_rows

    def columns(cut):
        return width * cut // UNITS // 128 * 128

    if n >= 4:
        mains = [[0] + [columns(cut) for cut in cuts] for cuts in MAINS]
        gives = [
            [cuts[-1]] + [columns(cut) for cut in ends[:-1]] + [width]
            for cuts, ends in zip(mains, GIVES)
        ]
    else:
        mains = [[0] + [columns(cut) for cut in (32, 64, 96)] + [width]] * 2
        gives = [[width]] * 2
    tail = max(width - cuts[-1] for cuts in mains) or 128
    slots = max(len(cuts) for cuts in mains)
    lanes = -(-rows // 128) * 128
    hbm = pl.BlockSpec(memory_space=pltpu.HBM)
    return pl.pallas_call(
        functools.partial(kernel, n, nf, mains, gives, GIVE_AT),
        out_shape=pltpu.VMEM((rows // nf, queries), jnp.float32),
        in_specs=[hbm] * 3 + [pl.BlockSpec(memory_space=pltpu.SMEM)],
        out_specs=pl.BlockSpec(memory_space=pltpu.VMEM),
        scratch_shapes=[
            pltpu.VMEM((q_rows, width), jnp.bfloat16),
            pltpu.VMEM((n, q_rows, width), jnp.bfloat16),
            pltpu.VMEM((rows, width), jnp.bfloat16),
            pltpu.VMEM((1, width), jnp.float32),
            pltpu.VMEM((1, width), jnp.float32),
            pltpu.VMEM((queries, lanes), jnp.float32),
            pltpu.VMEM((nf, rows // nf, queries), jnp.float32),
            pltpu.VMEM((2 * nf - 1, rows // nf, queries), jnp.float32),
            pltpu.VMEM((rows, tail), jnp.bfloat16),
            pltpu.VMEM((queries, tail), jnp.float32),
            pltpu.VMEM((rows, queries), jnp.float32),
            pltpu.VMEM((nf, rows // nf, queries), jnp.float32),
            pltpu.SemaphoreType.DMA((4,)),
            pltpu.SemaphoreType.DMA(((n - 1) * slots,)),
            pltpu.SemaphoreType.DMA((1,)),
            pltpu.SemaphoreType.DMA((max(1, max(len(ends) - 1 for ends in gives)),)),
            pltpu.SemaphoreType.REGULAR,
        ],
        compiler_params=pltpu.CompilerParams(collective_id=0, has_side_effects=True),
    )(train_grads, query_grads, curvature.reshape(1, width), row_counts)


def solution(mesh):
    placed = (
        P(("groups", "loop"), "feat"),
        P(("groups", "loop"), "feat"),
        P("feat"),
        P(("groups", "loop")),
    )
    return jax.shard_map(
        functools.partial(on_device, mesh.shape["loop"], mesh.shape["feat"]),
        mesh=mesh,
        in_specs=placed,
        out_specs=P(("groups", "loop", "feat"), None),
        check_vma=False,
    )
```

```python
import functools

import jax
import jax.numpy as jnp
from jax import lax
from jax.experimental import pallas as pl
from jax.experimental.pallas import tpu as pltpu
from jax.sharding import PartitionSpec as P

MESH = pl.DeviceIdType.MESH
damping_term = 0.1
MAINS = ((24, 48, 72, 95), (28, 57, 86, 115))
GIVES = ((115, 128), (128,))
GIVE_AT = (None, (2, 2))
UNITS = 128


def kernel(
    n, nf, mains, gives, give_at,
    t_hbm, q_hbm, c_hbm, count_ref, out_ref,
    q_ref, gath, t_ref, c_ref, inv_ref, acc, part, red, t_tail, p_tail, tail_acc, tail_part, tail_red,
    local_sem, recv_sem, share_sem, give_sem, ready_sem,
):
    me, f = lax.axis_index("loop"), lax.axis_index("feat")
    rows, width = t_ref.shape
    own_rows = rows // nf
    queries = out_ref.shape[1]
    tall = tail_part.shape[1]
    fold = own_rows // tall
    q_rows = q_ref.shape[0]
    slots = max(len(cuts) for cuts in mains)
    has_left, has_right = me > 0, me < n - 1
    is_first = me == 0
    is_end = is_first | (me == n - 1)
    is_helper = (me == 1) | (me == n - 2)
    head = max(cuts[1] for cuts in mains)

    load_q = [
        pltpu.make_async_copy(
            q_hbm.at[:, pl.ds(a, b - a)], q_ref.at[:, pl.ds(a, b - a)], local_sem.at[i]
        )
        for i, (a, b) in enumerate(((0, head), (head, width)))
    ]
    load_c = pltpu.make_async_copy(c_hbm, c_ref, local_sem.at[3])
    load_t = pltpu.make_async_copy(t_hbm, t_ref, local_sem.at[2])
    for load in load_q:
        load.start()

    barrier = pltpu.get_barrier_semaphore()

    @pl.when(has_right)
    def _():
        pl.semaphore_signal(barrier, inc=1, device_id={"loop": me + 1}, device_id_type=MESH)

    @pl.when(me == 1)
    def _():
        pl.semaphore_signal(barrier, inc=1, device_id={"loop": me - 1}, device_id_type=MESH)

    for k in range(1, nf):
        pl.semaphore_signal(
            barrier, inc=1, device_id={"feat": lax.rem(f + k, nf)}, device_id_type=MESH
        )
    load_c.start()
    load_t.start()
    acc[...] = jnp.zeros_like(acc)
    pl.semaphore_wait(barrier, jnp.where(is_first, has_right, has_left).astype(jnp.int32) + nf - 1)

    @pl.when(me > 1)
    def _():
        pl.semaphore_signal(ready_sem, inc=1, device_id={"loop": me - 1}, device_id_type=MESH)

    load_q[0].wait()

    def share(k):
        peer = lax.rem(f + k, nf)
        return pltpu.make_async_remote_copy(
            src_ref=part.at[peer],
            dst_ref=red.at[k - 1],
            send_sem=local_sem.at[2],
            recv_sem=share_sem.at[0],
            device_id={"feat": peer},
            device_id_type=MESH,
        )

    def tail_share(k):
        peer = lax.rem(f + k, nf)
        return pltpu.make_async_remote_copy(
            src_ref=tail_part.at[peer],
            dst_ref=tail_red.at[k],
            send_sem=local_sem.at[3],
            recv_sem=share_sem.at[1],
            device_id={"feat": peer, "loop": jnp.where(me == 1, 0, n - 1)},
            device_id_type=MESH,
        )

    def every(into, i):
        return pltpu.make_async_remote_copy(
            src_ref=into,
            dst_ref=into,
            send_sem=local_sem.at[2 + i],
            recv_sem=share_sem.at[i],
            device_id={"feat": lax.rem(f + 1, nf)},
            device_id_type=MESH,
        )

    def run(cuts, gift, give_when):
        count = len(cuts) - 1
        main = cuts[-1]
        tail = main < width

        def columns(piece):
            a = cuts[piece]
            b = cuts[piece + 1] if piece < count else width
            return pl.ds(a, b - a)

        def hop(way, block, piece, taker, own=False):
            span = gath.at[block, :, columns(piece)]
            slot = block - (block > taker).astype(jnp.int32)
            return pltpu.make_async_remote_copy(
                src_ref=q_ref.at[:, columns(piece)] if own else span,
                dst_ref=span,
                send_sem=local_sem.at[way],
                recv_sem=recv_sem.at[slot * slots + piece],
                device_id={"loop": jnp.clip(me + (2 * way - 1), 0, n - 1)},
                device_id_type=MESH,
            )

        def goes(way, piece):
            if piece < count:
                return has_right if way else has_left
            return me < n - 2 if way else me > 1

        def send_own(way, pieces):
            @pl.when(goes(way, pieces[0]))
            def _():
                for piece in pieces:
                    hop(way, me, piece, me + 2 * way - 1, own=True).start()

        def give(i):
            a, b = gift[i], gift[i + 1]
            return pltpu.make_async_remote_copy(
                src_ref=t_ref.at[:, pl.ds(a, b - a)],
                dst_ref=t_tail.at[:, pl.ds(a - main, b - a)],
                send_sem=local_sem.at[3],
                recv_sem=give_sem.at[i],
                device_id={"loop": jnp.where(is_first, 1, n - 2)},
                device_id_type=MESH,
            )

        def start_give():
            for i in range(len(gift) - 1):
                give(i).start()

        def multiply(block, piece, own=False):
            here = pl.ds(pl.multiple_of(block * q_rows, q_rows), q_rows)
            held = q_ref[:, columns(piece)] if own else gath[block, :, columns(piece)]
            exact = held.astype(jnp.float32) * inv_ref[:, columns(piece)]
            acc[here, 0:rows] += lax.dot_general(
                exact.astype(jnp.bfloat16), t_ref[:, columns(piece)], (((1,), (1,)), ((), ())),
                preferred_element_type=jnp.float32,
            )
            if piece == count:
                p_tail[here, 0:width - main] = exact

        def take(way, block, piece):
            hop(way, block, piece, me).wait_recv()

            @pl.when(goes(way, piece))
            def _():
                hop(way, block, piece, me + 2 * way - 1).start()

        def arrive(back, piece):
            from_left, from_right = me - back, me + back
            takes_left, takes_right = from_left >= 0, from_right < n

            @pl.when(takes_right)
            def _():
                take(0, from_right, piece)

            @pl.when(takes_left)
            def _():
                take(1, from_left, piece)

            @pl.loop(0, 2)
            def _(side):
                @pl.when(((side == 0) & takes_left) | ((side == 1) & takes_right))
                def _():
                    multiply(me + (2 * side - 1) * back, piece)

        send_own(0, [0])
        load_q[1].wait()
        send_own(0, range(1, count))
        if tail:
            @pl.when(me == n - 1)
            def _():
                send_own(0, [count])

        @pl.when(has_right & jnp.logical_not(is_first))
        def _():
            pl.semaphore_wait(ready_sem, 1)

        send_own(1, range(count))
        if tail:
            @pl.when(is_first)
            def _():
                send_own(1, [count])

        load_c.wait()
        load_t.wait()
        if tail and give_when is None:
            @pl.when(is_end)
            def _():
                start_give()

        inv_ref[...] = 1.0 / (damping_term + c_ref[...])
        for piece in range(count):
            multiply(me, piece, own=True)
        if tail:
            @pl.when(jnp.logical_not(is_end))
            def _():
                multiply(me, count, own=True)

        @pl.loop(1, n)
        def _(back):
            for piece in range(count):
                arrive(back, piece)
                if tail and give_when is not None and piece == give_when[1]:
                    @pl.when(is_end & (back == n - give_when[0]))
                    def _():
                        start_give()

            if tail:
                for way in range(2):
                    deep = me if way else n - 1 - me

                    @pl.when((back == deep) & jnp.logical_not(is_end))
                    def _():
                        send_own(way, [count])

                        @pl.loop(1, deep + 1)
                        def _(far):
                            block = me + (1 - 2 * way) * far
                            take(way, block, count)
                            multiply(block, count)

        turned = acc[...].T
        for k in range(nf):
            part[k] = turned[k * own_rows:(k + 1) * own_rows, 0:part.shape[2]]
        for k in range(1, nf):
            share(k).start()

        def tail_dot(i):
            at = pl.ds(gift[i] - main, gift[i + 1] - gift[i])
            return lax.dot_general(
                t_tail[:, at], p_tail[:, at].astype(jnp.bfloat16), (((1,), (1,)), ((), ())),
                preferred_element_type=jnp.float32,
            )

        if tail:
            @pl.when(is_helper)
            def _():
                total = None
                for i in range(len(gift) - 1):
                    give(i).wait_recv()
                    total = tail_dot(i) if total is None else tail_acc[...] + tail_dot(i)
                    if i < len(gift) - 2:
                        tail_acc[...] = total
                for k in range(nf):
                    tail_part[k] = jnp.concatenate(
                        [total[a:a + tall, :] for a in range(k * own_rows, (k + 1) * own_rows, tall)],
                        axis=1,
                    )
                for k in range(nf):
                    tail_share(k).start()

        def sent(way, blocks, wide):
            span = gath.at[pl.ds(0, blocks), :, pl.ds(0, wide)]
            pltpu.make_async_remote_copy(
                src_ref=span,
                dst_ref=span,
                send_sem=local_sem.at[way],
                recv_sem=recv_sem.at[0],
                device_id={"loop": jnp.clip(me + (2 * way - 1), 0, n - 1)},
                device_id_type=MESH,
            ).wait_send()

        for blocks in range(1, n):
            for way in range(2):
                @pl.when(me == (blocks - 1 if way else n - blocks))
                def _():
                    sent(way, blocks, width if blocks < n - 1 else main)

        if tail:
            @pl.when(is_end)
            def _():
                span = t_ref.at[:, pl.ds(main, width - main)]
                pltpu.make_async_remote_copy(
                    src_ref=span,
                    dst_ref=span,
                    send_sem=local_sem.at[3],
                    recv_sem=give_sem.at[0],
                    device_id={"loop": jnp.where(is_first, 1, n - 2)},
                    device_id_type=MESH,
                ).wait_send()

    if mains[0] == mains[1]:
        run(mains[0], gives[0], give_at[0])
    else:
        for parity in range(2):
            @pl.when(lax.rem(f, 2) == parity)
            def _():
                run(mains[parity], gives[parity], give_at[parity])

    live = f * own_rows + lax.broadcasted_iota(jnp.int32, out_ref.shape, 0) < count_ref[0]

    if mains[0][-1] < width:
        @pl.when(is_end)
        def _():
            every(tail_red, 1).wait_recv()
            more = tail_red[0]
            for k in range(1, nf):
                more = more + tail_red[k]
            out_ref[...] = part[f] + jnp.concatenate(
                [more[:, i * queries:(i + 1) * queries] for i in range(fold)], axis=0
            )

        @pl.when(jnp.logical_not(is_end))
        def _():
            out_ref[...] = part[f]
    else:
        out_ref[...] = part[f]

    every(red, 0).wait_recv()
    total = out_ref[...]
    for k in range(nf - 1):
        total = total + red[k]
    out_ref[...] = jnp.where(live, total, 0.0)
    every(red, 0).wait_send()
    if mains[0][-1] < width:
        @pl.when(is_helper)
        def _():
            every(tail_red, 1).wait_send()


def on_device(n, nf, train_grads, query_grads, curvature, row_counts):
    rows, width = train_grads.shape
    q_rows = query_grads.shape[0]
    queries = n * q_rows

    def columns(cut):
        return width * cut // UNITS // 128 * 128

    if n >= 4:
        mains = [[0] + [columns(cut) for cut in cuts] for cuts in MAINS]
        gives = [
            [cuts[-1]] + [columns(cut) for cut in ends[:-1]] + [width]
            for cuts, ends in zip(mains, GIVES)
        ]
    else:
        mains = [[0] + [columns(cut) for cut in (32, 64, 96)] + [width]] * 2
        gives = [[width]] * 2
    tail = max(width - cuts[-1] for cuts in mains) or 128
    slots = max(len(cuts) for cuts in mains)
    lanes = -(-rows // 128) * 128
    fold = max(1, min(128 // queries, rows // nf // 8))
    folded = (nf, rows // nf // fold, queries * fold)
    hbm = pl.BlockSpec(memory_space=pltpu.HBM)
    return pl.pallas_call(
        functools.partial(kernel, n, nf, mains, gives, GIVE_AT),
        out_shape=pltpu.VMEM((rows // nf, queries), jnp.float32),
        in_specs=[hbm] * 3 + [pl.BlockSpec(memory_space=pltpu.SMEM)],
        out_specs=pl.BlockSpec(memory_space=pltpu.VMEM),
        scratch_shapes=[
            pltpu.VMEM((q_rows, width), jnp.bfloat16),
            pltpu.VMEM((n, q_rows, width), jnp.bfloat16),
            pltpu.VMEM((rows, width), jnp.bfloat16),
            pltpu.VMEM((1, width), jnp.float32),
            pltpu.VMEM((1, width), jnp.float32),
            pltpu.VMEM((queries, lanes), jnp.float32),
            pltpu.VMEM((nf, rows // nf, queries), jnp.float32),
            pltpu.VMEM((nf - 1, rows // nf, queries), jnp.float32),
            pltpu.VMEM((rows, tail), jnp.bfloat16),
            pltpu.VMEM((queries, tail), jnp.float32),
            pltpu.VMEM((rows, queries), jnp.float32),
            pltpu.VMEM(folded, jnp.float32),
            pltpu.VMEM(folded, jnp.float32),
            pltpu.SemaphoreType.DMA((4,)),
            pltpu.SemaphoreType.DMA(((n - 1) * slots,)),
            pltpu.SemaphoreType.DMA((2,)),
            pltpu.SemaphoreType.DMA((max(1, max(len(ends) - 1 for ends in gives)),)),
            pltpu.SemaphoreType.REGULAR,
        ],
        compiler_params=pltpu.CompilerParams(collective_id=0, has_side_effects=True),
    )(train_grads, query_grads, curvature.reshape(1, width), row_counts)


def solution(mesh):
    placed = (
        P(("groups", "loop"), "feat"),
        P(("groups", "loop"), "feat"),
        P("feat"),
        P(("groups", "loop")),
    )
    return jax.shard_map(
        functools.partial(on_device, mesh.shape["loop"], mesh.shape["feat"]),
        mesh=mesh,
        in_specs=placed,
        out_specs=P(("groups", "loop", "feat"), None),
        check_vma=False,
    )
```

```python
import functools

import jax
import jax.numpy as jnp
from jax import lax
from jax.experimental import pallas as pl
from jax.experimental.pallas import tpu as pltpu
from jax.sharding import PartitionSpec as P

MESH = pl.DeviceIdType.MESH
damping_term = 0.1
MAINS = ((24, 48, 72, 95), (29, 58, 87, 115))
GIVE_AT = (None, (2, 2))
UNITS = 128


def kernel(
    n, nf, mains, give_at,
    t_hbm, q_hbm, c_hbm, count_ref, out_ref,
    q_ref, gath, t_ref, c_ref, inv_ref, acc, part, red, t_tail, p_tail, tail_part, tail_red,
    local_sem, recv_sem, share_sem, give_sem, ready_sem,
):
    me, f = lax.axis_index("loop"), lax.axis_index("feat")
    rows, width = t_ref.shape
    own_rows = rows // nf
    queries = out_ref.shape[1]
    tall = tail_part.shape[1]
    fold = own_rows // tall
    q_rows = q_ref.shape[0]
    slots = max(len(cuts) for cuts in mains)
    has_left, has_right = me > 0, me < n - 1
    is_first = me == 0
    is_end = is_first | (me == n - 1)
    is_helper = (me == 1) | (me == n - 2)
    head = max(cuts[1] for cuts in mains)

    load_q = [
        pltpu.make_async_copy(
            q_hbm.at[:, pl.ds(a, b - a)], q_ref.at[:, pl.ds(a, b - a)], local_sem.at[i]
        )
        for i, (a, b) in enumerate(((0, head), (head, width)))
    ]
    load_c = pltpu.make_async_copy(c_hbm, c_ref, local_sem.at[3])
    load_t = pltpu.make_async_copy(t_hbm, t_ref, local_sem.at[2])
    for load in load_q:
        load.start()

    barrier = pltpu.get_barrier_semaphore()

    @pl.when(has_right)
    def _():
        pl.semaphore_signal(barrier, inc=1, device_id={"loop": me + 1}, device_id_type=MESH)

    @pl.when(me == 1)
    def _():
        pl.semaphore_signal(barrier, inc=1, device_id={"loop": me - 1}, device_id_type=MESH)

    for k in range(1, nf):
        pl.semaphore_signal(
            barrier, inc=1, device_id={"feat": lax.rem(f + k, nf)}, device_id_type=MESH
        )
    load_c.start()
    load_t.start()
    acc[...] = jnp.zeros_like(acc)
    pl.semaphore_wait(barrier, jnp.where(is_first, has_right, has_left).astype(jnp.int32) + nf - 1)

    @pl.when(me > 1)
    def _():
        pl.semaphore_signal(ready_sem, inc=1, device_id={"loop": me - 1}, device_id_type=MESH)

    load_q[0].wait()

    def share(k):
        peer = lax.rem(f + k, nf)
        return pltpu.make_async_remote_copy(
            src_ref=part.at[peer],
            dst_ref=red.at[k - 1],
            send_sem=local_sem.at[2],
            recv_sem=share_sem.at[0],
            device_id={"feat": peer},
            device_id_type=MESH,
        )

    def tail_share(k):
        peer = lax.rem(f + k, nf)
        return pltpu.make_async_remote_copy(
            src_ref=tail_part.at[peer],
            dst_ref=tail_red.at[k],
            send_sem=local_sem.at[3],
            recv_sem=share_sem.at[1],
            device_id={"feat": peer, "loop": jnp.where(me == 1, 0, n - 1)},
            device_id_type=MESH,
        )

    def every(into, i):
        return pltpu.make_async_remote_copy(
            src_ref=into,
            dst_ref=into,
            send_sem=local_sem.at[2 + i],
            recv_sem=share_sem.at[i],
            device_id={"feat": lax.rem(f + 1, nf)},
            device_id_type=MESH,
        )

    def run(cuts, give_when):
        count = len(cuts) - 1
        main = cuts[-1]
        tail = main < width

        def columns(piece):
            a = cuts[piece]
            b = cuts[piece + 1] if piece < count else width
            return pl.ds(a, b - a)

        def hop(way, block, piece, taker, own=False):
            span = gath.at[block, :, columns(piece)]
            slot = block - (block > taker).astype(jnp.int32)
            return pltpu.make_async_remote_copy(
                src_ref=q_ref.at[:, columns(piece)] if own else span,
                dst_ref=span,
                send_sem=local_sem.at[way],
                recv_sem=recv_sem.at[slot * slots + piece],
                device_id={"loop": jnp.clip(me + (2 * way - 1), 0, n - 1)},
                device_id_type=MESH,
            )

        def goes(way, piece):
            if piece < count:
                return has_right if way else has_left
            return me < n - 2 if way else me > 1

        def send_own(way, pieces):
            @pl.when(goes(way, pieces[0]))
            def _():
                for piece in pieces:
                    hop(way, me, piece, me + 2 * way - 1, own=True).start()

        def give():
            return pltpu.make_async_remote_copy(
                src_ref=t_ref.at[:, pl.ds(main, width - main)],
                dst_ref=t_tail.at[:, pl.ds(0, width - main)],
                send_sem=local_sem.at[3],
                recv_sem=give_sem.at[0],
                device_id={"loop": jnp.where(is_first, 1, n - 2)},
                device_id_type=MESH,
            )

        def multiply(block, piece, own=False):
            here = pl.ds(pl.multiple_of(block * q_rows, q_rows), q_rows)
            held = q_ref[:, columns(piece)] if own else gath[block, :, columns(piece)]
            exact = held.astype(jnp.float32) * inv_ref[:, columns(piece)]
            acc[here, 0:rows] += lax.dot_general(
                exact.astype(jnp.bfloat16), t_ref[:, columns(piece)], (((1,), (1,)), ((), ())),
                preferred_element_type=jnp.float32,
            )
            if piece == count:
                p_tail[here, 0:width - main] = exact

        def take(way, block, piece):
            hop(way, block, piece, me).wait_recv()

            @pl.when(goes(way, piece))
            def _():
                hop(way, block, piece, me + 2 * way - 1).start()

        def arrive(back, piece):
            from_left, from_right = me - back, me + back
            takes_left, takes_right = from_left >= 0, from_right < n

            @pl.when(takes_right)
            def _():
                take(0, from_right, piece)

            @pl.when(takes_left)
            def _():
                take(1, from_left, piece)

            @pl.loop(0, 2)
            def _(side):
                @pl.when(((side == 0) & takes_left) | ((side == 1) & takes_right))
                def _():
                    multiply(me + (2 * side - 1) * back, piece)

        send_own(0, [0])
        load_q[1].wait()
        send_own(0, range(1, count))
        if tail:
            @pl.when(me == n - 1)
            def _():
                send_own(0, [count])

        @pl.when(has_right & jnp.logical_not(is_first))
        def _():
            pl.semaphore_wait(ready_sem, 1)

        send_own(1, range(count))
        if tail:
            @pl.when(is_first)
            def _():
                send_own(1, [count])

        load_c.wait()
        load_t.wait()
        if tail and give_when is None:
            @pl.when(is_end)
            def _():
                give().start()

        inv_ref[...] = 1.0 / (damping_term + c_ref[...])
        for piece in range(count):
            multiply(me, piece, own=True)
        if tail:
            @pl.when(jnp.logical_not(is_end))
            def _():
                multiply(me, count, own=True)

        @pl.loop(1, n)
        def _(back):
            for piece in range(count):
                arrive(back, piece)
                if tail and give_when is not None and piece == give_when[1]:
                    @pl.when(is_end & (back == n - give_when[0]))
                    def _():
                        give().start()

            if tail:
                for way in range(2):
                    deep = me if way else n - 1 - me

                    @pl.when((back == deep) & jnp.logical_not(is_end))
                    def _():
                        send_own(way, [count])

                        @pl.loop(1, deep + 1)
                        def _(far):
                            block = me + (1 - 2 * way) * far
                            take(way, block, count)
                            multiply(block, count)

        turned = acc[...].T
        for k in range(nf):
            part[k] = turned[k * own_rows:(k + 1) * own_rows, 0:part.shape[2]]
        for k in range(1, nf):
            share(k).start()

        if tail:
            @pl.when(is_helper)
            def _():
                give().wait_recv()
                total = lax.dot_general(
                    t_tail[:, 0:width - main], p_tail[:, 0:width - main].astype(jnp.bfloat16),
                    (((1,), (1,)), ((), ())), preferred_element_type=jnp.float32,
                )
                for k in range(nf):
                    tail_part[k] = jnp.concatenate(
                        [total[a:a + tall, :] for a in range(k * own_rows, (k + 1) * own_rows, tall)],
                        axis=1,
                    )
                for k in range(nf):
                    tail_share(k).start()

        def sent(way, blocks, wide):
            span = gath.at[pl.ds(0, blocks), :, pl.ds(0, wide)]
            pltpu.make_async_remote_copy(
                src_ref=span,
                dst_ref=span,
                send_sem=local_sem.at[way],
                recv_sem=recv_sem.at[0],
                device_id={"loop": jnp.clip(me + (2 * way - 1), 0, n - 1)},
                device_id_type=MESH,
            ).wait_send()

        for blocks in range(1, n):
            for way in range(2):
                @pl.when(me == (blocks - 1 if way else n - blocks))
                def _():
                    sent(way, blocks, width if blocks < n - 1 else main)

        if tail:
            @pl.when(is_end)
            def _():
                give().wait_send()

    if mains[0] == mains[1]:
        run(mains[0], give_at[0])
    else:
        for parity in range(2):
            @pl.when(lax.rem(f, 2) == parity)
            def _():
                run(mains[parity], give_at[parity])

    live = f * own_rows + lax.broadcasted_iota(jnp.int32, out_ref.shape, 0) < count_ref[0]

    if mains[0][-1] < width:
        @pl.when(is_end)
        def _():
            every(tail_red, 1).wait_recv()
            more = tail_red[0]
            for k in range(1, nf):
                more = more + tail_red[k]
            out_ref[...] = part[f] + jnp.concatenate(
                [more[:, i * queries:(i + 1) * queries] for i in range(fold)], axis=0
            )

        @pl.when(jnp.logical_not(is_end))
        def _():
            out_ref[...] = part[f]
    else:
        out_ref[...] = part[f]

    every(red, 0).wait_recv()
    total = out_ref[...]
    for k in range(nf - 1):
        total = total + red[k]
    out_ref[...] = jnp.where(live, total, 0.0)
    every(red, 0).wait_send()
    if mains[0][-1] < width:
        @pl.when(is_helper)
        def _():
            every(tail_red, 1).wait_send()


def on_device(n, nf, train_grads, query_grads, curvature, row_counts):
    rows, width = train_grads.shape
    q_rows = query_grads.shape[0]
    queries = n * q_rows

    def columns(cut):
        return width * cut // UNITS // 128 * 128

    if n >= 4:
        mains = [[0] + [columns(cut) for cut in cuts] for cuts in MAINS]
    else:
        mains = [[0] + [columns(cut) for cut in (32, 64, 96)] + [width]] * 2
    tail = max(width - cuts[-1] for cuts in mains) or 128
    slots = max(len(cuts) for cuts in mains)
    lanes = -(-rows // 128) * 128
    fold = max(1, min(128 // queries, rows // nf // 8))
    folded = (nf, rows // nf // fold, queries * fold)
    hbm = pl.BlockSpec(memory_space=pltpu.HBM)
    return pl.pallas_call(
        functools.partial(kernel, n, nf, mains, GIVE_AT),
        out_shape=pltpu.VMEM((rows // nf, queries), jnp.float32),
        in_specs=[hbm] * 3 + [pl.BlockSpec(memory_space=pltpu.SMEM)],
        out_specs=pl.BlockSpec(memory_space=pltpu.VMEM),
        scratch_shapes=[
            pltpu.VMEM((q_rows, width), jnp.bfloat16),
            pltpu.VMEM((n, q_rows, width), jnp.bfloat16),
            pltpu.VMEM((rows, width), jnp.bfloat16),
            pltpu.VMEM((1, width), jnp.float32),
            pltpu.VMEM((1, width), jnp.float32),
            pltpu.VMEM((queries, lanes), jnp.float32),
            pltpu.VMEM((nf, rows // nf, queries), jnp.float32),
            pltpu.VMEM((nf - 1, rows // nf, queries), jnp.float32),
            pltpu.VMEM((rows, tail), jnp.bfloat16),
            pltpu.VMEM((queries, tail), jnp.float32),
            pltpu.VMEM(folded, jnp.float32),
            pltpu.VMEM(folded, jnp.float32),
            pltpu.SemaphoreType.DMA((4,)),
            pltpu.SemaphoreType.DMA(((n - 1) * slots,)),
            pltpu.SemaphoreType.DMA((2,)),
            pltpu.SemaphoreType.DMA((1,)),
            pltpu.SemaphoreType.REGULAR,
        ],
        compiler_params=pltpu.CompilerParams(collective_id=0, has_side_effects=True),
    )(train_grads, query_grads, curvature.reshape(1, width), row_counts)


def solution(mesh):
    placed = (
        P(("groups", "loop"), "feat"),
        P(("groups", "loop"), "feat"),
        P("feat"),
        P(("groups", "loop")),
    )
    return jax.shard_map(
        functools.partial(on_device, mesh.shape["loop"], mesh.shape["feat"]),
        mesh=mesh,
        in_specs=placed,
        out_specs=P(("groups", "loop", "feat"), None),
        check_vma=False,
    )
```

```python
import functools

import jax
import jax.numpy as jnp
from jax import lax
from jax.experimental import pallas as pl
from jax.experimental.pallas import tpu as pltpu
from jax.sharding import PartitionSpec as P

MESH = pl.DeviceIdType.MESH
damping_term = 0.1
MAINS = ((24, 48, 72, 95), (29, 58, 87, 115))
GIVE_AT = (None, (2, 2))
UNITS = 128


def kernel(
    n, nf, mains, give_at,
    t_hbm, q_hbm, c_hbm, count_ref, out_ref,
    q_ref, gath, t_ref, c_ref, inv_ref, acc, part, red, t_tail, p_tail, tail_part, tail_red,
    local_sem, recv_sem, share_sem, give_sem, ready_sem,
):
    me, f = lax.axis_index("loop"), lax.axis_index("feat")
    rows, width = t_ref.shape
    own_rows = rows // nf
    queries = out_ref.shape[1]
    tall = tail_part.shape[1]
    fold = own_rows // tall
    q_rows = q_ref.shape[0]
    slots = max(len(cuts) for cuts in mains)
    has_left, has_right = me > 0, me < n - 1
    is_first = me == 0
    is_end = is_first | (me == n - 1)
    is_helper = (me == 1) | (me == n - 2)
    head = max(cuts[1] for cuts in mains)

    load_q = [
        pltpu.make_async_copy(
            q_hbm.at[:, pl.ds(a, b - a)], q_ref.at[:, pl.ds(a, b - a)], local_sem.at[i]
        )
        for i, (a, b) in enumerate(((0, head), (head, width)))
    ]
    load_c = pltpu.make_async_copy(c_hbm, c_ref, local_sem.at[3])
    load_t = pltpu.make_async_copy(t_hbm, t_ref, local_sem.at[2])
    for load in load_q:
        load.start()

    barrier = pltpu.get_barrier_semaphore()

    @pl.when(has_right)
    def _():
        pl.semaphore_signal(barrier, inc=1, device_id={"loop": me + 1}, device_id_type=MESH)

    @pl.when(me == 1)
    def _():
        pl.semaphore_signal(barrier, inc=1, device_id={"loop": me - 1}, device_id_type=MESH)

    for k in range(1, nf):
        pl.semaphore_signal(
            barrier, inc=1, device_id={"feat": lax.rem(f + k, nf)}, device_id_type=MESH
        )
    load_c.start()
    load_t.start()
    acc[...] = jnp.zeros_like(acc)
    pl.semaphore_wait(barrier, jnp.where(is_first, has_right, has_left).astype(jnp.int32) + nf - 1)

    @pl.when(me > 1)
    def _():
        pl.semaphore_signal(ready_sem, inc=1, device_id={"loop": me - 1}, device_id_type=MESH)

    load_q[0].wait()

    def share(k):
        peer = lax.rem(f + k, nf)
        return pltpu.make_async_remote_copy(
            src_ref=part.at[peer],
            dst_ref=red.at[k - 1],
            send_sem=local_sem.at[2],
            recv_sem=share_sem.at[0],
            device_id={"feat": peer},
            device_id_type=MESH,
        )

    def tail_share(k):
        peer = lax.rem(f + k, nf)
        return pltpu.make_async_remote_copy(
            src_ref=tail_part.at[peer],
            dst_ref=tail_red.at[k],
            send_sem=local_sem.at[3],
            recv_sem=share_sem.at[1],
            device_id={"feat": peer, "loop": jnp.where(me == 1, 0, n - 1)},
            device_id_type=MESH,
        )

    def every(into, i):
        return pltpu.make_async_remote_copy(
            src_ref=into,
            dst_ref=into,
            send_sem=local_sem.at[2 + i],
            recv_sem=share_sem.at[i],
            device_id={"feat": lax.rem(f + 1, nf)},
            device_id_type=MESH,
        )

    def run(cuts, give_when):
        count = len(cuts) - 1
        main = cuts[-1]
        tail = main < width

        def columns(piece):
            a = cuts[piece]
            b = cuts[piece + 1] if piece < count else width
            return pl.ds(a, b - a)

        def hop(way, block, piece, taker, own=False):
            span = gath.at[block, :, columns(piece)]
            slot = block - (block > taker).astype(jnp.int32)
            return pltpu.make_async_remote_copy(
                src_ref=q_ref.at[:, columns(piece)] if own else span,
                dst_ref=span,
                send_sem=local_sem.at[way],
                recv_sem=recv_sem.at[slot * slots + piece],
                device_id={"loop": jnp.clip(me + (2 * way - 1), 0, n - 1)},
                device_id_type=MESH,
            )

        def goes(way, piece):
            if piece < count:
                return has_right if way else has_left
            return me < n - 2 if way else me > 1

        def send_own(way, pieces):
            @pl.when(goes(way, pieces[0]))
            def _():
                for piece in pieces:
                    hop(way, me, piece, me + 2 * way - 1, own=True).start()

        def give():
            return pltpu.make_async_remote_copy(
                src_ref=t_ref.at[:, pl.ds(main, width - main)],
                dst_ref=t_tail.at[:, pl.ds(0, width - main)],
                send_sem=local_sem.at[3],
                recv_sem=give_sem.at[0],
                device_id={"loop": jnp.where(is_first, 1, n - 2)},
                device_id_type=MESH,
            )

        def multiply(block, piece, own=False):
            here = pl.ds(pl.multiple_of(block * q_rows, q_rows), q_rows)
            held = q_ref[:, columns(piece)] if own else gath[block, :, columns(piece)]
            exact = held.astype(jnp.float32) * inv_ref[:, columns(piece)]
            acc[here, 0:rows] += lax.dot_general(
                exact.astype(jnp.bfloat16), t_ref[:, columns(piece)], (((1,), (1,)), ((), ())),
                preferred_element_type=jnp.float32,
            )
            if piece == count:
                p_tail[here, 0:width - main] = exact

        def take(way, block, piece):
            hop(way, block, piece, me).wait_recv()

            @pl.when(goes(way, piece))
            def _():
                hop(way, block, piece, me + 2 * way - 1).start()

        def arrive(back, piece):
            from_left, from_right = me - back, me + back
            takes_left, takes_right = from_left >= 0, from_right < n

            @pl.when(takes_right)
            def _():
                take(0, from_right, piece)

            @pl.when(takes_left)
            def _():
                take(1, from_left, piece)

            @pl.loop(0, 2)
            def _(side):
                @pl.when(((side == 0) & takes_left) | ((side == 1) & takes_right))
                def _():
                    multiply(me + (2 * side - 1) * back, piece)

        send_own(0, [0])
        load_q[1].wait()
        send_own(0, range(1, count))
        if tail:
            @pl.when(me == n - 1)
            def _():
                send_own(0, [count])

        @pl.when(has_right & jnp.logical_not(is_first))
        def _():
            pl.semaphore_wait(ready_sem, 1)

        send_own(1, range(count))
        if tail:
            @pl.when(is_first)
            def _():
                send_own(1, [count])

        load_c.wait()
        load_t.wait()
        if tail and give_when is None:
            @pl.when(is_end)
            def _():
                give().start()

        inv_ref[...] = 1.0 / (damping_term + c_ref[...])
        for piece in range(count):
            multiply(me, piece, own=True)
        if tail:
            @pl.when(jnp.logical_not(is_end))
            def _():
                multiply(me, count, own=True)

        @pl.loop(1, n)
        def _(back):
            for piece in range(count):
                arrive(back, piece)
                if tail and give_when is not None and piece == give_when[1]:
                    @pl.when(is_end & (back == n - give_when[0]))
                    def _():
                        give().start()

            if tail:
                for way in range(2):
                    deep = me if way else n - 1 - me

                    @pl.when((back == deep) & jnp.logical_not(is_end))
                    def _():
                        send_own(way, [count])

                        @pl.loop(1, deep + 1)
                        def _(far):
                            block = me + (1 - 2 * way) * far
                            take(way, block, count)
                            multiply(block, count)

        turned = acc[...].T
        for k in range(nf):
            part[k] = turned[k * own_rows:(k + 1) * own_rows, 0:part.shape[2]]
        for k in [*range(2, nf), 1]:
            share(k).start()

        if tail:
            @pl.when(is_helper)
            def _():
                give().wait_recv()
                total = lax.dot_general(
                    t_tail[:, 0:width - main], p_tail[:, 0:width - main].astype(jnp.bfloat16),
                    (((1,), (1,)), ((), ())), preferred_element_type=jnp.float32,
                )
                for k in range(nf):
                    tail_part[k] = jnp.concatenate(
                        [total[a:a + tall, :] for a in range(k * own_rows, (k + 1) * own_rows, tall)],
                        axis=1,
                    )
                for k in range(nf):
                    tail_share(k).start()

        def sent(way, blocks, wide):
            span = gath.at[pl.ds(0, blocks), :, pl.ds(0, wide)]
            pltpu.make_async_remote_copy(
                src_ref=span,
                dst_ref=span,
                send_sem=local_sem.at[way],
                recv_sem=recv_sem.at[0],
                device_id={"loop": jnp.clip(me + (2 * way - 1), 0, n - 1)},
                device_id_type=MESH,
            ).wait_send()

        for blocks in range(1, n):
            for way in range(2):
                @pl.when(me == (blocks - 1 if way else n - blocks))
                def _():
                    sent(way, blocks, width if blocks < n - 1 else main)

        if tail:
            @pl.when(is_end)
            def _():
                give().wait_send()

    if mains[0] == mains[1]:
        run(mains[0], give_at[0])
    else:
        for parity in range(2):
            @pl.when(lax.rem(f, 2) == parity)
            def _():
                run(mains[parity], give_at[parity])

    live = f * own_rows + lax.broadcasted_iota(jnp.int32, out_ref.shape, 0) < count_ref[0]

    if mains[0][-1] < width:
        @pl.when(is_end)
        def _():
            every(tail_red, 1).wait_recv()
            more = tail_red[0]
            for k in range(1, nf):
                more = more + tail_red[k]
            out_ref[...] = part[f] + jnp.concatenate(
                [more[:, i * queries:(i + 1) * queries] for i in range(fold)], axis=0
            )

        @pl.when(jnp.logical_not(is_end))
        def _():
            out_ref[...] = part[f]
    else:
        out_ref[...] = part[f]

    every(red, 0).wait_recv()
    total = out_ref[...]
    for k in range(nf - 1):
        total = total + red[k]
    out_ref[...] = jnp.where(live, total, 0.0)
    every(red, 0).wait_send()
    if mains[0][-1] < width:
        @pl.when(is_helper)
        def _():
            every(tail_red, 1).wait_send()


def on_device(n, nf, train_grads, query_grads, curvature, row_counts):
    rows, width = train_grads.shape
    q_rows = query_grads.shape[0]
    queries = n * q_rows

    def columns(cut):
        return width * cut // UNITS // 128 * 128

    if n >= 4:
        mains = [[0] + [columns(cut) for cut in cuts] for cuts in MAINS]
    else:
        mains = [[0] + [columns(cut) for cut in (32, 64, 96)] + [width]] * 2
    tail = max(width - cuts[-1] for cuts in mains) or 128
    slots = max(len(cuts) for cuts in mains)
    lanes = -(-rows // 128) * 128
    fold = max(1, min(128 // queries, rows // nf // 8))
    folded = (nf, rows // nf // fold, queries * fold)
    hbm = pl.BlockSpec(memory_space=pltpu.HBM)
    return pl.pallas_call(
        functools.partial(kernel, n, nf, mains, GIVE_AT),
        out_shape=pltpu.VMEM((rows // nf, queries), jnp.float32),
        in_specs=[hbm] * 3 + [pl.BlockSpec(memory_space=pltpu.SMEM)],
        out_specs=pl.BlockSpec(memory_space=pltpu.VMEM),
        scratch_shapes=[
            pltpu.VMEM((q_rows, width), jnp.bfloat16),
            pltpu.VMEM((n, q_rows, width), jnp.bfloat16),
            pltpu.VMEM((rows, width), jnp.bfloat16),
            pltpu.VMEM((1, width), jnp.float32),
            pltpu.VMEM((1, width), jnp.float32),
            pltpu.VMEM((queries, lanes), jnp.float32),
            pltpu.VMEM((nf, rows // nf, queries), jnp.float32),
            pltpu.VMEM((nf - 1, rows // nf, queries), jnp.float32),
            pltpu.VMEM((rows, tail), jnp.bfloat16),
            pltpu.VMEM((queries, tail), jnp.float32),
            pltpu.VMEM(folded, jnp.float32),
            pltpu.VMEM(folded, jnp.float32),
            pltpu.SemaphoreType.DMA((4,)),
            pltpu.SemaphoreType.DMA(((n - 1) * slots,)),
            pltpu.SemaphoreType.DMA((2,)),
            pltpu.SemaphoreType.DMA((1,)),
            pltpu.SemaphoreType.REGULAR,
        ],
        compiler_params=pltpu.CompilerParams(collective_id=0, has_side_effects=True),
    )(train_grads, query_grads, curvature.reshape(1, width), row_counts)


def solution(mesh):
    placed = (
        P(("groups", "loop"), "feat"),
        P(("groups", "loop"), "feat"),
        P("feat"),
        P(("groups", "loop")),
    )
    return jax.shard_map(
        functools.partial(on_device, mesh.shape["loop"], mesh.shape["feat"]),
        mesh=mesh,
        in_specs=placed,
        out_specs=P(("groups", "loop", "feat"), None),
        check_vma=False,
    )
```

```python
import functools

import jax
import jax.numpy as jnp
from jax import lax
from jax.experimental import pallas as pl
from jax.experimental.pallas import tpu as pltpu
from jax.sharding import PartitionSpec as P

MESH = pl.DeviceIdType.MESH
damping_term = 0.1
MAINS = ((24, 48, 72, 94), (29, 58, 87, 116))
GIVE_AT = (None, (2, 2))
UNITS = 128


def kernel(
    n, nf, mains, give_at,
    t_hbm, q_hbm, c_hbm, count_ref, out_ref,
    q_ref, gath, t_ref, c_ref, inv_ref, acc, part, red, t_tail, p_tail, tail_part, tail_red,
    local_sem, recv_sem, share_sem, give_sem, ready_sem,
):
    me, f = lax.axis_index("loop"), lax.axis_index("feat")
    rows, width = t_ref.shape
    own_rows = rows // nf
    queries = out_ref.shape[1]
    tall = tail_part.shape[1]
    fold = own_rows // tall
    q_rows = q_ref.shape[0]
    slots = max(len(cuts) for cuts in mains)
    has_left, has_right = me > 0, me < n - 1
    is_first = me == 0
    is_end = is_first | (me == n - 1)
    is_helper = (me == 1) | (me == n - 2)
    head = max(cuts[1] for cuts in mains)

    load_q = [
        pltpu.make_async_copy(
            q_hbm.at[:, pl.ds(a, b - a)], q_ref.at[:, pl.ds(a, b - a)], local_sem.at[i]
        )
        for i, (a, b) in enumerate(((0, head), (head, width)))
    ]
    load_c = pltpu.make_async_copy(c_hbm, c_ref, local_sem.at[3])
    load_t = pltpu.make_async_copy(t_hbm, t_ref, local_sem.at[2])
    for load in load_q:
        load.start()

    barrier = pltpu.get_barrier_semaphore()

    @pl.when(has_right)
    def _():
        pl.semaphore_signal(barrier, inc=1, device_id={"loop": me + 1}, device_id_type=MESH)

    @pl.when(me == 1)
    def _():
        pl.semaphore_signal(barrier, inc=1, device_id={"loop": me - 1}, device_id_type=MESH)

    for k in range(1, nf):
        pl.semaphore_signal(
            barrier, inc=1, device_id={"feat": lax.rem(f + k, nf)}, device_id_type=MESH
        )
    load_c.start()
    load_t.start()
    acc[...] = jnp.zeros_like(acc)
    pl.semaphore_wait(barrier, jnp.where(is_first, has_right, has_left).astype(jnp.int32) + nf - 1)

    @pl.when(me > 1)
    def _():
        pl.semaphore_signal(ready_sem, inc=1, device_id={"loop": me - 1}, device_id_type=MESH)

    load_q[0].wait()

    def share(k):
        peer = lax.rem(f + k, nf)
        return pltpu.make_async_remote_copy(
            src_ref=part.at[peer],
            dst_ref=red.at[k - 1],
            send_sem=local_sem.at[2],
            recv_sem=share_sem.at[0],
            device_id={"feat": peer},
            device_id_type=MESH,
        )

    def tail_share(k):
        peer = lax.rem(f + k, nf)
        return pltpu.make_async_remote_copy(
            src_ref=tail_part.at[peer],
            dst_ref=tail_red.at[k],
            send_sem=local_sem.at[3],
            recv_sem=share_sem.at[1],
            device_id={"feat": peer, "loop": jnp.where(me == 1, 0, n - 1)},
            device_id_type=MESH,
        )

    def every(into, i):
        return pltpu.make_async_remote_copy(
            src_ref=into,
            dst_ref=into,
            send_sem=local_sem.at[2 + i],
            recv_sem=share_sem.at[i],
            device_id={"feat": lax.rem(f + 1, nf)},
            device_id_type=MESH,
        )

    def run(cuts, give_when):
        count = len(cuts) - 1
        main = cuts[-1]
        tail = main < width

        def columns(piece):
            a = cuts[piece]
            b = cuts[piece + 1] if piece < count else width
            return pl.ds(a, b - a)

        def hop(way, block, piece, taker, own=False):
            span = gath.at[block, :, columns(piece)]
            slot = block - (block > taker).astype(jnp.int32)
            return pltpu.make_async_remote_copy(
                src_ref=q_ref.at[:, columns(piece)] if own else span,
                dst_ref=span,
                send_sem=local_sem.at[way],
                recv_sem=recv_sem.at[slot * slots + piece],
                device_id={"loop": jnp.clip(me + (2 * way - 1), 0, n - 1)},
                device_id_type=MESH,
            )

        def goes(way, piece):
            if piece < count:
                return has_right if way else has_left
            return me < n - 2 if way else me > 1

        def send_own(way, pieces):
            @pl.when(goes(way, pieces[0]))
            def _():
                for piece in pieces:
                    hop(way, me, piece, me + 2 * way - 1, own=True).start()

        def give():
            return pltpu.make_async_remote_copy(
                src_ref=t_ref.at[:, pl.ds(main, width - main)],
                dst_ref=t_tail.at[:, pl.ds(0, width - main)],
                send_sem=local_sem.at[3],
                recv_sem=give_sem.at[0],
                device_id={"loop": jnp.where(is_first, 1, n - 2)},
                device_id_type=MESH,
            )

        def multiply(block, piece, own=False):
            here = pl.ds(pl.multiple_of(block * q_rows, q_rows), q_rows)
            held = q_ref[:, columns(piece)] if own else gath[block, :, columns(piece)]
            exact = held.astype(jnp.float32) * inv_ref[:, columns(piece)]
            acc[here, 0:rows] += lax.dot_general(
                exact.astype(jnp.bfloat16), t_ref[:, columns(piece)], (((1,), (1,)), ((), ())),
                preferred_element_type=jnp.float32,
            )
            if piece == count:
                p_tail[here, 0:width - main] = exact

        def take(way, block, piece):
            hop(way, block, piece, me).wait_recv()

            @pl.when(goes(way, piece))
            def _():
                hop(way, block, piece, me + 2 * way - 1).start()

        def arrive(back, piece):
            from_left, from_right = me - back, me + back
            takes_left, takes_right = from_left >= 0, from_right < n

            @pl.when(takes_right)
            def _():
                take(0, from_right, piece)

            @pl.when(takes_left)
            def _():
                take(1, from_left, piece)

            @pl.loop(0, 2)
            def _(side):
                @pl.when(((side == 0) & takes_left) | ((side == 1) & takes_right))
                def _():
                    multiply(me + (2 * side - 1) * back, piece)

        send_own(0, [0])
        load_q[1].wait()
        send_own(0, range(1, count))
        if tail:
            @pl.when(me == n - 1)
            def _():
                send_own(0, [count])

        @pl.when(has_right & jnp.logical_not(is_first))
        def _():
            pl.semaphore_wait(ready_sem, 1)

        send_own(1, range(count))
        if tail:
            @pl.when(is_first)
            def _():
                send_own(1, [count])

        load_c.wait()
        load_t.wait()
        if tail and give_when is None:
            @pl.when(is_end)
            def _():
                give().start()

        inv_ref[...] = 1.0 / (damping_term + c_ref[...])
        for piece in range(count):
            multiply(me, piece, own=True)
        if tail:
            @pl.when(jnp.logical_not(is_end))
            def _():
                multiply(me, count, own=True)

        @pl.loop(1, n)
        def _(back):
            for piece in range(count):
                arrive(back, piece)
                if tail and give_when is not None and piece == give_when[1]:
                    @pl.when(is_end & (back == n - give_when[0]))
                    def _():
                        give().start()

            if tail:
                for way in range(2):
                    deep = me if way else n - 1 - me

                    @pl.when((back == deep) & jnp.logical_not(is_end))
                    def _():
                        send_own(way, [count])

                        @pl.loop(1, deep + 1)
                        def _(far):
                            block = me + (1 - 2 * way) * far
                            take(way, block, count)
                            multiply(block, count)

        turned = acc[...].T
        for k in range(nf):
            part[k] = turned[k * own_rows:(k + 1) * own_rows, 0:part.shape[2]]
        for k in [*range(2, nf), 1]:
            share(k).start()

        if tail:
            @pl.when(is_helper)
            def _():
                give().wait_recv()
                total = lax.dot_general(
                    t_tail[:, 0:width - main], p_tail[:, 0:width - main].astype(jnp.bfloat16),
                    (((1,), (1,)), ((), ())), preferred_element_type=jnp.float32,
                )
                for k in range(nf):
                    tail_part[k] = jnp.concatenate(
                        [total[a:a + tall, :] for a in range(k * own_rows, (k + 1) * own_rows, tall)],
                        axis=1,
                    )
                for k in range(nf):
                    tail_share(k).start()

        def sent(way, blocks, wide):
            span = gath.at[pl.ds(0, blocks), :, pl.ds(0, wide)]
            pltpu.make_async_remote_copy(
                src_ref=span,
                dst_ref=span,
                send_sem=local_sem.at[way],
                recv_sem=recv_sem.at[0],
                device_id={"loop": jnp.clip(me + (2 * way - 1), 0, n - 1)},
                device_id_type=MESH,
            ).wait_send()

        for blocks in range(1, n):
            for way in range(2):
                @pl.when(me == (blocks - 1 if way else n - blocks))
                def _():
                    sent(way, blocks, width if blocks < n - 1 else main)

        if tail:
            @pl.when(is_end)
            def _():
                give().wait_send()

    if mains[0] == mains[1]:
        run(mains[0], give_at[0])
    else:
        for parity in range(2):
            @pl.when(lax.rem(f, 2) == parity)
            def _():
                run(mains[parity], give_at[parity])

    live = f * own_rows + lax.broadcasted_iota(jnp.int32, out_ref.shape, 0) < count_ref[0]

    if mains[0][-1] < width:
        @pl.when(is_end)
        def _():
            every(tail_red, 1).wait_recv()
            more = tail_red[0]
            for k in range(1, nf):
                more = more + tail_red[k]
            out_ref[...] = part[f] + jnp.concatenate(
                [more[:, i * queries:(i + 1) * queries] for i in range(fold)], axis=0
            )

        @pl.when(jnp.logical_not(is_end))
        def _():
            out_ref[...] = part[f]
    else:
        out_ref[...] = part[f]

    every(red, 0).wait_recv()
    total = out_ref[...]
    for k in range(nf - 1):
        total = total + red[k]
    out_ref[...] = jnp.where(live, total, 0.0)
    every(red, 0).wait_send()
    if mains[0][-1] < width:
        @pl.when(is_helper)
        def _():
            every(tail_red, 1).wait_send()


def on_device(n, nf, train_grads, query_grads, curvature, row_counts):
    rows, width = train_grads.shape
    q_rows = query_grads.shape[0]
    queries = n * q_rows

    def columns(cut):
        return width * cut // UNITS // 128 * 128

    if n >= 4:
        mains = [[0] + [columns(cut) for cut in cuts] for cuts in MAINS]
    else:
        mains = [[0] + [columns(cut) for cut in (32, 64, 96)] + [width]] * 2
    tail = max(width - cuts[-1] for cuts in mains) or 128
    slots = max(len(cuts) for cuts in mains)
    lanes = -(-rows // 128) * 128
    fold = max(1, min(128 // queries, rows // nf // 8))
    folded = (nf, rows // nf // fold, queries * fold)
    hbm = pl.BlockSpec(memory_space=pltpu.HBM)
    return pl.pallas_call(
        functools.partial(kernel, n, nf, mains, GIVE_AT),
        out_shape=pltpu.VMEM((rows // nf, queries), jnp.float32),
        in_specs=[hbm] * 3 + [pl.BlockSpec(memory_space=pltpu.SMEM)],
        out_specs=pl.BlockSpec(memory_space=pltpu.VMEM),
        scratch_shapes=[
            pltpu.VMEM((q_rows, width), jnp.bfloat16),
            pltpu.VMEM((n, q_rows, width), jnp.bfloat16),
            pltpu.VMEM((rows, width), jnp.bfloat16),
            pltpu.VMEM((1, width), jnp.float32),
            pltpu.VMEM((1, width), jnp.float32),
            pltpu.VMEM((queries, lanes), jnp.float32),
            pltpu.VMEM((nf, rows // nf, queries), jnp.float32),
            pltpu.VMEM((nf - 1, rows // nf, queries), jnp.float32),
            pltpu.VMEM((rows, tail), jnp.bfloat16),
            pltpu.VMEM((queries, tail), jnp.float32),
            pltpu.VMEM(folded, jnp.float32),
            pltpu.VMEM(folded, jnp.float32),
            pltpu.SemaphoreType.DMA((4,)),
            pltpu.SemaphoreType.DMA(((n - 1) * slots,)),
            pltpu.SemaphoreType.DMA((2,)),
            pltpu.SemaphoreType.DMA((1,)),
            pltpu.SemaphoreType.REGULAR,
        ],
        compiler_params=pltpu.CompilerParams(collective_id=0, has_side_effects=True),
    )(train_grads, query_grads, curvature.reshape(1, width), row_counts)


def solution(mesh):
    placed = (
        P(("groups", "loop"), "feat"),
        P(("groups", "loop"), "feat"),
        P("feat"),
        P(("groups", "loop")),
    )
    return jax.shard_map(
        functools.partial(on_device, mesh.shape["loop"], mesh.shape["feat"]),
        mesh=mesh,
        in_specs=placed,
        out_specs=P(("groups", "loop", "feat"), None),
        check_vma=False,
    )
```
